32 devices in a mesh: member: 4 (over y, x), space: 8 (over z, core).
Axes of the slice: x: 2, y: 2, z: 4, core: 2. Of those that a mesh axis runs over, the one named last changes fastest.
Arguments:
- hidden_codes: bfloat16 [8, 256, 23040], P('member', None, 'space'), may hold values from -6 to 6
- w_in: bfloat16 [1024, 256], replicated, may hold values from -0.375 to 0.375
- b_in: float32 [1024], replicated, may hold values from -3 to 3
- w_out: bfloat16 [72, 1024], replicated, may hold values from -0.1875 to 0.1875
- b_out: float32 [72], replicated, may hold values from -3 to 3
- target: bfloat16 [72, 23040], P(None, 'space'), may hold values from -6 to 6
- band_start: int32 [8], P('space'), may hold values from 0 to 14, as said below
Outputs:
- code_sensitivity: bfloat16 [8, 256, 23040], P('member', None, 'space')
- grad_w_in: float32 [1024, 256], replicated
- grad_w_out: float32 [72, 1024], replicated
- grad_b_in: float32 [1024], replicated
The draws below stay inside these ranges and needn't reach their ends.
Inputs may be any that keep to these rules, and one draw needn't show every extreme that they name: band_start holds each of 0, 2, 4, ... once, in some order.
All inputs are finite; a program needn't handle non-finite values.
Results may differ from the reference program's by a relative error of at most 0.005.
The reference program's roundings to bfloat16 on the way count: a program that leaves them out, or rounds other values in their place, can miss the bound.
Values may be sent and summed in bfloat16 or wider, within the bound.
A program may use at most 128 MiB of HBM per device.

```python
import math
import jax
import jax.numpy as jnp
from jax import lax

CHANNELS = 72
HID = 1024
LATENT = 256
LON = 1440
ROWS_DEV = 2
MEMBERS = 8
CELLS = 23040
N_SPACE = 8


def draw_band_start(key, part):
    order = jax.random.permutation(jax.random.fold_in(key, 11), N_SPACE)
    return (order * ROWS_DEV).astype(jnp.int32)


def level_of(rng, dims, cuts, smallest, high):
    def one(dim, parts):
        heights = jax.random.uniform(jax.random.fold_in(jax.random.fold_in(rng, 6), dim), (parts,), jnp.float32, smallest / len(cuts), high / len(cuts))
        return jnp.repeat(jnp.exp(heights), dims[dim] // parts).reshape((-1,) + (1,) * (len(dims) - dim - 1))

    level = one(*cuts[0])
    for cut in cuts[1:]:
        level = level * one(*cut)
    return level


def bell_draw(rng, dims, scale, reach, split=(), kind=jnp.bfloat16):
    factor_of = level_of(rng, dims, split, -0.22, 0.18) if split else 1.0
    values = jax.random.normal(rng, dims, jnp.float32) * scale * factor_of
    return jnp.minimum(jnp.maximum(values, -reach), reach).astype(kind)


def setup_inputs(seed: int = 0) -> dict:
    key_list = jax.random.split(jax.random.key(seed), 8)
    hidden_codes = bell_draw(key_list[0], (MEMBERS, LATENT, CELLS), 1.0, 6.0, ((0, 4), (2, 8)))
    w_in = bell_draw(key_list[1], (HID, LATENT), LATENT ** -0.5, 0.375)
    b_in = bell_draw(key_list[2], (HID,), 0.5, 3.0, (), jnp.float32)
    w_out = bell_draw(key_list[3], (CHANNELS, HID), HID ** -0.5, 0.1875)
    b_out = bell_draw(key_list[4], (CHANNELS,), 0.5, 3.0, (), jnp.float32)
    target = bell_draw(key_list[5], (CHANNELS, CELLS), 1.0, 6.0, ((1, 8),))
    band_start = draw_band_start(jax.random.fold_in(key_list[7], 71), 0)
    return dict(hidden_codes=hidden_codes, w_in=w_in, b_in=b_in, w_out=w_out, b_out=b_out, target=target, band_start=band_start)


def slope(diff):
    return diff / jnp.sqrt(diff * diff + 0.0625)

def area_weights(band_start):
    rows = band_start[:, None] + jnp.arange(ROWS_DEV, dtype=jnp.int32)[None, :]
    angle = (rows.astype(jnp.float32) + 0.5) * (math.pi / (ROWS_DEV * N_SPACE)) - math.pi / 2
    return jnp.repeat(jnp.cos(angle).reshape(-1), LON)

def reference(hidden_codes, w_in, b_in, w_out, b_out, target, band_start):
    area = area_weights(band_start)
    members = hidden_codes.shape[0]
    cells = hidden_codes.shape[2]

    def apply_readout(inputs):
        pre = jnp.dot(w_in, inputs, preferred_element_type=jnp.float32) + b_in[:, None]
        act = jax.nn.gelu(pre).astype(jnp.bfloat16)
        return (jnp.dot(w_out, act, preferred_element_type=jnp.float32) + b_out[:, None]).astype(jnp.bfloat16)
    predicted_maps = lax.map(apply_readout, hidden_codes)
    goal = target.astype(jnp.float32)

    def cross_sensitivity(mine):
        diagonal_contribution = mine.astype(jnp.float32)

        def lone_realization(total, other):
            return (total + slope(diagonal_contribution - other.astype(jnp.float32)), None)
        couple_index, discarded_value = lax.scan(lone_realization, jnp.zeros_like(diagonal_contribution), predicted_maps)
        return (area[None, :] * (slope(diagonal_contribution - goal) - couple_index / members)).astype(jnp.bfloat16)
    prediction_sensitivity = lax.map(cross_sensitivity, predicted_maps)

    def reverse_sweep(carry, items):
        inputs, prediction_adjoint = items
        pre = jnp.dot(w_in, inputs, preferred_element_type=jnp.float32) + b_in[:, None]
        act_f, undo = jax.vjp(jax.nn.gelu, pre)
        act = act_f.astype(jnp.bfloat16)
        dact = jnp.dot(w_out.T, prediction_adjoint, preferred_element_type=jnp.float32)
        dpre = undo(dact)[0].astype(jnp.bfloat16)
        dlat = jnp.dot(w_in.T, dpre, preferred_element_type=jnp.float32).astype(jnp.bfloat16)
        adjoint_entry_matrix = carry[0] + jnp.dot(dpre, inputs.T, preferred_element_type=jnp.float32)
        adjoint_exit_matrix = carry[1] + jnp.dot(prediction_adjoint, act.T, preferred_element_type=jnp.float32)
        adjoint_offset = carry[2] + lax.optimization_barrier(jnp.sum(dpre.astype(jnp.float32), axis=1))
        return ((adjoint_entry_matrix, adjoint_exit_matrix, adjoint_offset), dlat)
    opening_offset = (jnp.zeros(w_in.shape, jnp.float32), jnp.zeros(w_out.shape, jnp.float32), jnp.zeros(b_in.shape, jnp.float32))
    (adjoint_entry_matrix, adjoint_exit_matrix, adjoint_offset), code_sensitivity = lax.scan(reverse_sweep, opening_offset, (hidden_codes, prediction_sensitivity))
    scale = 1.0 / math.sqrt(members * (cells // N_SPACE))
    return (code_sensitivity, adjoint_entry_matrix * scale, adjoint_exit_matrix * scale, adjoint_offset * scale)
```

```python
import functools
import math

import jax
import jax.numpy as jnp
from jax import lax
from jax.experimental import pallas as pl
from jax.experimental.pallas import tpu as pltpu
from jax.sharding import PartitionSpec as P

LON = 1440
HB = 256
MESH = pl.DeviceIdType.MESH
NT = (((1,), (1,)), ((), ()))
F32 = jnp.float32
BF16 = jnp.bfloat16
K0 = math.sqrt(2.0 / math.pi)
K1 = K0 * 0.044715


def slope(diff):
    return diff * lax.rsqrt(diff * diff + 0.0625)


def kernel(
    msize,
    ssize,
    cells,
    hid_ref,
    w_in_ref,
    w_in_t_ref,
    b_in_ref,
    w_out_ref,
    w_out_t_ref,
    b_out_ref,
    tgt_ref,
    area_ref,
    code_ref,
    gwi_ref,
    gwo_ref,
    gb_ref,
    hid,
    tgt,
    act,
    dgelu,
    fcs,
    fcr,
    dfs,
    dfr,
    acc_i,
    acc_o,
    acc_b,
    half,
    r1,
    s2,
    r2,
    r3,
    full,
    x1s,
    x1r,
    x2s,
    x2r,
    p1,
    p2s,
    p2r,
    p3s,
    p3r,
    p4s,
    p4r,
    p5s,
    p5r,
):
    local = hid_ref.shape[0]
    hidden = w_in_ref.shape[0]
    latent = w_in_ref.shape[1]
    chans = w_out_ref.shape[0]
    width = hid.shape[3]
    blocks = hidden // HB
    members = local * msize
    zsize = ssize // 2
    me = lax.axis_index("member")
    sp = lax.axis_index("space")
    core = lax.rem(sp, 2)
    z = sp // 2
    partner = z * 2 + (1 - core)

    def mpeer(k):
        return lax.rem(me + k, msize)

    def zpeer(k):
        return lax.rem(z + k, zsize) * 2 + core

    barrier = pltpu.get_barrier_semaphore()
    pl.semaphore_signal(barrier, inc=1, device_id=(me, partner), device_id_type=MESH)
    for k in range(1, msize):
        pl.semaphore_signal(barrier, inc=1, device_id=(mpeer(k), sp), device_id_type=MESH)
    for k in range(1, zsize):
        pl.semaphore_signal(barrier, inc=1, device_id=(me, zpeer(k)), device_id_type=MESH)

    for c in range(msize):
        lo = c * width
        n = min(width, cells - lo)
        if n < width:
            hid[c] = jnp.zeros(hid.shape[1:], BF16)
            tgt[c] = jnp.zeros(tgt.shape[1:], BF16)
        for m in range(local):
            hid[c, m, :, :n] = hid_ref[m, :, lo : lo + n]
        tgt[c, :, :n] = tgt_ref[:, lo : lo + n]
    acc_i[...] = jnp.zeros_like(acc_i)
    acc_o[...] = jnp.zeros_like(acc_o)
    acc_b[...] = jnp.zeros_like(acc_b)

    def x1(k):
        return pltpu.make_async_remote_copy(
            src_ref=fcs.at[mpeer(k)],
            dst_ref=fcr.at[me],
            send_sem=x1s.at[k],
            recv_sem=x1r.at[k],
            device_id=(mpeer(k), sp),
            device_id_type=MESH,
        )

    def x2(k):
        return pltpu.make_async_remote_copy(
            src_ref=dfs.at[mpeer(k)],
            dst_ref=dfr.at[me],
            send_sem=x2s.at[k],
            recv_sem=x2r.at[k],
            device_id=(mpeer(k), sp),
            device_id_type=MESH,
        )

    def forward(c):
        for m in range(local):

            def block(h, carry):
                rows = pl.ds(pl.multiple_of(h * HB, HB), HB)
                x = jnp.dot(w_in_ref[rows, :], hid[c, m], preferred_element_type=F32)
                x = x + b_in_ref[rows, :]
                u = x * x
                t = jnp.tanh(x * (K0 + K1 * u))
                hx = 0.5 * x
                act[c, m, rows, :] = (hx + hx * t).astype(BF16)
                dgelu[c, m, rows, :] = (0.5 + 0.5 * t) + (hx * (1.0 - t * t)) * (
                    K0 + (3.0 * K1) * u
                )
                return carry

            lax.fori_loop(0, blocks, block, 0)
            fc = jnp.dot(w_out_ref[...], act[c, m], preferred_element_type=F32)
            fcs[c, m] = (fc + b_out_ref[...]).astype(BF16)

    def step(k, carry):
        forward(mpeer(k))

        @pl.when(k == 1)
        def _():
            pl.semaphore_wait(barrier, msize + zsize - 1)

        x1(k).start()
        return carry

    lax.fori_loop(1, msize, step, 0)
    forward(me)
    fcr[me] = fcs[me]
    for k in range(1, msize):
        x1(k).wait()

    def pairs(i, carry):
        lanes = pl.ds(pl.multiple_of(i * 128, 128), 128)
        vals = [fcr[q // local, q % local, :, lanes].astype(F32) for q in range(members)]
        total = [jnp.zeros_like(vals[0]) for q in range(members)]
        for a in range(members):
            for b in range(a + 1, members):
                s = slope(vals[a] - vals[b])
                total[a] = total[a] + s
                total[b] = total[b] - s
        goal = tgt[me, :, lanes].astype(F32)
        weight = area_ref[me, :, lanes]
        for q in range(members):
            d = weight * (slope(vals[q] - goal) - total[q] * (1.0 / members))
            dfs[q // local, q % local, :, lanes] = d.astype(BF16)
        return carry

    lax.fori_loop(0, width // 128, pairs, 0)
    for k in range(1, msize):
        x2(k).start()
    dfr[me] = dfs[me]

    def backward(c):
        for m in range(local):
            df = dfr[c, m]

            def block(h, carry):
                rows = pl.ds(pl.multiple_of(h * HB, HB), HB)
                acc_o[rows, :chans] += lax.dot_general(
                    act[c, m, rows, :], df, NT, preferred_element_type=F32
                )
                da = jnp.dot(w_out_t_ref[rows, :], df, preferred_element_type=F32)
                dp = (da * dgelu[c, m, rows, :]).astype(BF16)
                act[c, m, rows, :] = dp
                acc_i[rows, :] += lax.dot_general(
                    dp, hid[c, m], NT, preferred_element_type=F32
                )
                dpf = dp.astype(F32)
                tot = dpf[:, :128]
                for i in range(1, width // 128):
                    tot = tot + dpf[:, i * 128 : (i + 1) * 128]
                acc_b[rows, :] += tot
                return carry

            lax.fori_loop(0, blocks, block, 0)

    backward(me)

    def bstep(k, carry):
        x2(k).wait()
        backward(lax.rem(me + msize - k, msize))
        return carry

    lax.fori_loop(1, msize, bstep, 0)

    todo = [(c, m) for c in range(msize) for m in range(local)]

    def back_to_codes(count):
        for _ in range(min(count, len(todo))):
            c, m = todo.pop(0)
            lo = c * width
            n = min(width, cells - lo)
            d = jnp.dot(w_in_t_ref[...], act[c, m], preferred_element_type=F32)
            code_ref[m, :, lo : lo + n] = d[:, :n].astype(BF16)

    nrows = hidden // 2
    piece = nrows // msize

    def collect(start):
        rows = pl.ds(pl.multiple_of(start, nrows), nrows)
        bias = jnp.sum(acc_b[rows, :], axis=1, keepdims=True)
        lane = lax.broadcasted_iota(jnp.int32, (nrows, 128), 1)
        right = jnp.where(lane == chans, bias, 0.0)
        return rows, right

    def right_of(start):
        rows, bias = collect(start)
        return acc_i[rows, :], acc_o[rows, :] + bias

    li, lr = right_of((1 - core) * nrows)
    half[:, :latent] = li.astype(BF16)
    half[:, latent:] = lr.astype(BF16)
    c1 = pltpu.make_async_remote_copy(
        src_ref=half,
        dst_ref=r1,
        send_sem=p1.at[0],
        recv_sem=p1.at[1],
        device_id=(me, partner),
        device_id_type=MESH,
    )
    c1.start()
    back_to_codes(1)
    c1.wait()
    mi, mr = right_of(core * nrows)
    s2[:, :, :latent] = (mi + r1[:, :latent].astype(F32)).astype(BF16).reshape(
        msize, piece, latent
    )
    s2[:, :, latent:] = (mr + r1[:, latent:].astype(F32)).astype(BF16).reshape(
        msize, piece, 128
    )
    moves = []
    for k in range(1, msize):
        moves.append(
            pltpu.make_async_remote_copy(
                src_ref=s2.at[mpeer(k)],
                dst_ref=r2.at[k],
                send_sem=p2s.at[k],
                recv_sem=p2r.at[k],
                device_id=(mpeer(k), sp),
                device_id_type=MESH,
            )
        )
        moves[-1].start()
    back_to_codes(len(todo) // 2)
    for copy in moves:
        copy.wait()
    summed = s2[me].astype(F32)
    for k in range(1, msize):
        summed = summed + r2[k].astype(F32)
    r3[z] = summed.astype(BF16)
    moves = []
    for k in range(1, zsize):
        moves.append(
            pltpu.make_async_remote_copy(
                src_ref=r3.at[z],
                dst_ref=r3.at[z],
                send_sem=p3s.at[k],
                recv_sem=p3r.at[k],
                device_id=(me, zpeer(k)),
                device_id_type=MESH,
            )
        )
        moves[-1].start()
    back_to_codes(len(todo))
    for copy in moves:
        copy.wait()
    summed = r3[0].astype(F32)
    for k in range(1, zsize):
        summed = summed + r3[k].astype(F32)
    full[core, me] = summed.astype(BF16)

    def share(k):
        return pltpu.make_async_remote_copy(
            src_ref=full.at[core, me],
            dst_ref=full.at[core, me],
            send_sem=p4s.at[k],
            recv_sem=p4r.at[k],
            device_id=(mpeer(k), sp),
            device_id_type=MESH,
        )

    def across(k):
        owner = lax.rem(me + msize - k, msize)
        return pltpu.make_async_remote_copy(
            src_ref=full.at[core, owner],
            dst_ref=full.at[core, owner],
            send_sem=p5s.at[k],
            recv_sem=p5r.at[k],
            device_id=(me, partner),
            device_id_type=MESH,
        )

    for k in range(1, msize):
        share(k).start()
    across(0).start()
    for k in range(1, msize):
        share(k).wait()
        across(k).start()
    for k in range(msize):
        across(k).wait()
    scale = 1.0 / math.sqrt(members * cells)
    for side in range(2):
        for m in range(msize):
            lo = side * nrows + m * piece
            gwi_ref[lo : lo + piece, :] = full[side, m, :, :latent].astype(F32) * scale
            acc_o[lo : lo + piece, :] = full[side, m, :, latent:].astype(F32) * scale
    turned = jnp.transpose(acc_o[...])
    gwo_ref[...] = turned[:chans]
    gb_ref[...] = turned[chans : chans + 1]


def on_device(hidden_codes, w_in, b_in, w_out, b_out, target, band_start):
    local, latent, cells = hidden_codes.shape
    hidden = w_in.shape[0]
    chans = w_out.shape[0]
    msize = lax.axis_size("member")
    ssize = lax.axis_size("space")
    zsize = ssize // 2
    rows = cells // LON
    lat_rows = rows * ssize
    tiles = -(-cells // 128)
    width = -(-tiles // msize) * 128
    place = jnp.arange(msize * width, dtype=jnp.int32)
    angle = ((band_start[0] + place // LON).astype(F32) + 0.5) * (
        math.pi / lat_rows
    ) - math.pi / 2
    area = jnp.where(place < cells, jnp.cos(angle), 0.0).reshape(msize, 1, width)
    nrows = hidden // 2
    piece = nrows // msize
    wide = latent + 128
    vmem = pl.BlockSpec(memory_space=pltpu.VMEM)
    dma = pltpu.SemaphoreType.DMA
    code, gwi, gwo, gb = pl.pallas_call(
        functools.partial(kernel, msize, ssize, cells),
        out_shape=(
            jax.ShapeDtypeStruct((local, latent, cells), BF16),
            jax.ShapeDtypeStruct((hidden, latent), F32),
            jax.ShapeDtypeStruct((chans, hidden), F32),
            jax.ShapeDtypeStruct((1, hidden), F32),
        ),
        in_specs=[vmem] * 9,
        out_specs=(vmem,) * 4,
        scratch_shapes=[
            pltpu.VMEM((msize, local, latent, width), BF16),
            pltpu.VMEM((msize, chans, width), BF16),
            pltpu.VMEM((msize, local, hidden, width), BF16),
            pltpu.VMEM((msize, local, hidden, width), F32),
            pltpu.VMEM((msize, local, chans, width), BF16),
            pltpu.VMEM((msize, local, chans, width), BF16),
            pltpu.VMEM((msize, local, chans, width), BF16),
            pltpu.VMEM((msize, local, chans, width), BF16),
            pltpu.VMEM((hidden, latent), F32),
            pltpu.VMEM((hidden, 128), F32),
            pltpu.VMEM((hidden, 128), F32),
            pltpu.VMEM((nrows, wide), BF16),
            pltpu.VMEM((nrows, wide), BF16),
            pltpu.VMEM((msize, piece, wide), BF16),
            pltpu.VMEM((msize, piece, wide), BF16),
            pltpu.VMEM((zsize, piece, wide), BF16),
            pltpu.VMEM((2, msize, piece, wide), BF16),
            dma((msize,)),
            dma((msize,)),
            dma((msize,)),
            dma((msize,)),
            dma((2,)),
            dma((msize,)),
            dma((msize,)),
            dma((zsize,)),
            dma((zsize,)),
            dma((msize,)),
            dma((msize,)),
            dma((msize,)),
            dma((msize,)),
        ],
        compiler_params=pltpu.CompilerParams(
            collective_id=0, has_side_effects=True, vmem_limit_bytes=67043328
        ),
    )(
        hidden_codes,
        w_in,
        w_in.T,
        b_in[:, None],
        w_out,
        w_out.T,
        b_out[:, None],
        target,
        area,
    )
    return code, gwi, gwo, gb[0]


def solution(mesh):
    in_specs = (P("member", None, "space"), P(), P(), P(), P(), P(None, "space"), P("space"))
    out_specs = (P("member", None, "space"), P(), P(), P())
    return jax.shard_map(
        on_device, mesh=mesh, in_specs=in_specs, out_specs=out_specs, check_vma=False
    )
```

```python
import functools
import math

import jax
import jax.numpy as jnp
from jax import lax
from jax.experimental import pallas as pl
from jax.experimental.pallas import tpu as pltpu
from jax.sharding import PartitionSpec as P

LON = 1440
HB = 256
MESH = pl.DeviceIdType.MESH
NT = (((1,), (1,)), ((), ()))
F32 = jnp.float32
BF16 = jnp.bfloat16
K0 = math.sqrt(2.0 / math.pi)
K1 = K0 * 0.044715


def slope(diff):
    return diff * lax.rsqrt(diff * diff + 0.0625)


def kernel(
    msize,
    ssize,
    cells,
    hid_ref,
    w_in_ref,
    b_in_ref,
    w_out_ref,
    b_out_ref,
    tgt_ref,
    area_ref,
    code_ref,
    gwi_ref,
    gwo_ref,
    gb_ref,
    hid,
    tgt,
    act,
    dgelu,
    fcs,
    fcr,
    dfs,
    dfr,
    acc_i,
    acc_o,
    acc_b,
    half,
    r1,
    s2,
    r2,
    r3,
    full,
    x1s,
    x1r,
    x2s,
    x2r,
    p1,
    p2s,
    p2r,
    p3s,
    p3r,
    p4s,
    p4r,
    p5s,
    p5r,
    w_in_t,
    w_out_t,
    b_in,
    b_out,
    load,
    save,
):
    local = hid_ref.shape[0]
    hidden = w_in_ref.shape[0]
    latent = w_in_ref.shape[1]
    chans = w_out_ref.shape[0]
    width = hid.shape[2]
    blocks = hidden // HB
    members = local * msize
    zsize = ssize // 2
    me = lax.axis_index("member")
    sp = lax.axis_index("space")
    core = lax.rem(sp, 2)
    z = sp // 2
    partner = z * 2 + (1 - core)

    def mpeer(k):
        return lax.rem(me + k, msize)

    def zpeer(k):
        return lax.rem(z + k, zsize) * 2 + core

    barrier = pltpu.get_barrier_semaphore()
    pl.semaphore_signal(barrier, inc=1, device_id=(me, partner), device_id_type=MESH)
    for k in range(1, msize):
        pl.semaphore_signal(barrier, inc=1, device_id=(mpeer(k), sp), device_id_type=MESH)
    for k in range(1, zsize):
        pl.semaphore_signal(barrier, inc=1, device_id=(me, zpeer(k)), device_id_type=MESH)

    last = msize - 1
    rest = cells - last * width

    def span(c):
        return width if c < last else rest

    def fetch(c, m, n, lo):
        return pltpu.make_async_copy(
            hid_ref.at[m, pl.ds(lo, n)], hid.at[c, m, pl.ds(0, n)], load.at[c, m]
        )

    def put(c, m):
        n = span(c)
        return pltpu.make_async_copy(
            hid.at[c, m, pl.ds(0, n)], code_ref.at[m, pl.ds(c * width, n)], save.at[c, m]
        )

    for c in range(msize):
        for m in range(local):
            fetch(c, m, span(c), c * width).start()
    if rest < width:
        hid[last, :, rest:, :] = jnp.zeros((local, width - rest, latent), BF16)
        tgt[last] = jnp.zeros(tgt.shape[1:], BF16)
    for c in range(msize):
        n = span(c)
        tgt[c, :, :n] = tgt_ref[:, c * width : c * width + n]
    b_in[...] = jnp.transpose(jnp.broadcast_to(b_in_ref[...], (128, hidden)))
    b_out[...] = jnp.transpose(jnp.broadcast_to(b_out_ref[...], (128, chans)))
    acc_i[...] = jnp.zeros_like(acc_i)
    acc_o[...] = jnp.zeros_like(acc_o)
    acc_b[...] = jnp.zeros_like(acc_b)

    def x1(k):
        return pltpu.make_async_remote_copy(
            src_ref=fcs.at[mpeer(k)],
            dst_ref=fcr.at[me],
            send_sem=x1s.at[k],
            recv_sem=x1r.at[k],
            device_id=(mpeer(k), sp),
            device_id_type=MESH,
        )

    def x2(k):
        return pltpu.make_async_remote_copy(
            src_ref=dfs.at[mpeer(k)],
            dst_ref=dfr.at[me],
            send_sem=x2s.at[k],
            recv_sem=x2r.at[k],
            device_id=(mpeer(k), sp),
            device_id_type=MESH,
        )

    def forward(c):
        for m in range(local):

            @pl.when(c < last)
            def _():
                fetch(c, m, width, 0).wait()

            @pl.when(c == last)
            def _():
                fetch(c, m, rest, 0).wait()

            def block(h, carry):
                rows = pl.ds(pl.multiple_of(h * HB, HB), HB)
                x = lax.dot_general(
                    w_in_ref[rows, :], hid[c, m], NT, preferred_element_type=F32
                )
                x = x + b_in[rows, :1]
                u = x * x
                s = 0.5 + 0.5 * jnp.tanh(x * (K0 + K1 * u))
                g = x * s
                act[c, m, rows, :] = g.astype(BF16)
                dgelu[c, m, rows, :] = s + (g * (1.0 - s)) * (2.0 * K0 + (6.0 * K1) * u)
                return carry

            lax.fori_loop(0, blocks, block, 0)
            fc = jnp.dot(w_out_ref[...], act[c, m], preferred_element_type=F32)
            fcs[c, m] = (fc + b_out[:, :1]).astype(BF16)

    def step(k, carry):
        forward(mpeer(k))

        @pl.when(k == 1)
        def _():
            pl.semaphore_wait(barrier, msize + zsize - 1)

        x1(k).start()
        return carry

    lax.fori_loop(1, msize, step, 0)
    forward(me)
    fcr[me] = fcs[me]
    w_in_t[...] = jnp.transpose(w_in_ref[...])
    w_out_t[...] = jnp.transpose(w_out_ref[...].astype(F32)).astype(BF16)
    for k in range(1, msize):
        x1(k).wait()

    def pairs(i, carry):
        lanes = pl.ds(pl.multiple_of(i * 128, 128), 128)
        vals = [fcr[q // local, q % local, :, lanes].astype(F32) for q in range(members)]
        total = [jnp.zeros_like(vals[0]) for q in range(members)]
        for a in range(members):
            for b in range(a + 1, members):
                s = slope(vals[a] - vals[b])
                total[a] = total[a] + s
                total[b] = total[b] - s
        goal = tgt[me, :, lanes].astype(F32)
        weight = area_ref[me, :, lanes]
        for q in range(members):
            d = weight * (slope(vals[q] - goal) - total[q] * (1.0 / members))
            dfs[q // local, q % local, :, lanes] = d.astype(BF16)
        return carry

    lax.fori_loop(0, width // 128, pairs, 0)
    for k in range(1, msize):
        x2(k).start()
    dfr[me] = dfs[me]

    def backward(c):
        for m in range(local):
            df = dfr[c, m]

            def block(h, carry):
                rows = pl.ds(pl.multiple_of(h * HB, HB), HB)
                acc_o[rows, :chans] += lax.dot_general(
                    act[c, m, rows, :], df, NT, preferred_element_type=F32
                )
                da = jnp.dot(w_out_t[rows, :], df, preferred_element_type=F32)
                dp = (da * dgelu[c, m, rows, :]).astype(BF16)
                act[c, m, rows, :] = dp
                acc_i[rows, :] += jnp.dot(dp, hid[c, m], preferred_element_type=F32)
                dpf = dp.astype(F32)
                tot = dpf[:, :128]
                for i in range(1, width // 128):
                    tot = tot + dpf[:, i * 128 : (i + 1) * 128]
                acc_b[rows, :] += tot
                return carry

            lax.fori_loop(0, blocks, block, 0)

    backward(me)

    def bstep(k, carry):
        x2(k).wait()
        backward(lax.rem(me + msize - k, msize))
        return carry

    lax.fori_loop(1, msize, bstep, 0)

    todo = [(c, m) for c in range(msize) for m in range(local)]

    def back_to_codes(count):
        for _ in range(min(count, len(todo))):
            c, m = todo.pop(0)
            d = jnp.dot(w_in_t[...], act[c, m], preferred_element_type=F32)
            hid[c, m] = jnp.transpose(d.astype(BF16))
            put(c, m).start()

    nrows = hidden // 2
    piece = nrows // msize

    def collect(start):
        rows = pl.ds(pl.multiple_of(start, nrows), nrows)
        bias = jnp.sum(acc_b[rows, :], axis=1, keepdims=True)
        lane = lax.broadcasted_iota(jnp.int32, (nrows, 128), 1)
        right = jnp.where(lane == chans, bias, 0.0)
        return rows, right

    def right_of(start):
        rows, bias = collect(start)
        return acc_i[rows, :], acc_o[rows, :] + bias

    li, lr = right_of((1 - core) * nrows)
    half[:, :latent] = li.astype(BF16)
    half[:, latent:] = lr.astype(BF16)
    c1 = pltpu.make_async_remote_copy(
        src_ref=half,
        dst_ref=r1,
        send_sem=p1.at[0],
        recv_sem=p1.at[1],
        device_id=(me, partner),
        device_id_type=MESH,
    )
    c1.start()
    back_to_codes(1)
    c1.wait()
    mi, mr = right_of(core * nrows)
    s2[:, :, :latent] = (mi + r1[:, :latent].astype(F32)).astype(BF16).reshape(
        msize, piece, latent
    )
    s2[:, :, latent:] = (mr + r1[:, latent:].astype(F32)).astype(BF16).reshape(
        msize, piece, 128
    )
    moves = []
    for k in range(1, msize):
        moves.append(
            pltpu.make_async_remote_copy(
                src_ref=s2.at[mpeer(k)],
                dst_ref=r2.at[k],
                send_sem=p2s.at[k],
                recv_sem=p2r.at[k],
                device_id=(mpeer(k), sp),
                device_id_type=MESH,
            )
        )
        moves[-1].start()
    back_to_codes(len(todo) // 2)
    for copy in moves:
        copy.wait()
    summed = s2[me].astype(F32)
    for k in range(1, msize):
        summed = summed + r2[k].astype(F32)
    r3[z] = summed.astype(BF16)
    moves = []
    for k in range(1, zsize):
        moves.append(
            pltpu.make_async_remote_copy(
                src_ref=r3.at[z],
                dst_ref=r3.at[z],
                send_sem=p3s.at[k],
                recv_sem=p3r.at[k],
                device_id=(me, zpeer(k)),
                device_id_type=MESH,
            )
        )
        moves[-1].start()
    back_to_codes(len(todo))
    for copy in moves:
        copy.wait()
    summed = r3[0].astype(F32)
    for k in range(1, zsize):
        summed = summed + r3[k].astype(F32)
    full[core, me] = summed.astype(BF16)

    def share(k):
        return pltpu.make_async_remote_copy(
            src_ref=full.at[core, me],
            dst_ref=full.at[core, me],
            send_sem=p4s.at[k],
            recv_sem=p4r.at[k],
            device_id=(mpeer(k), sp),
            device_id_type=MESH,
        )

    def across(k):
        owner = lax.rem(me + msize - k, msize)
        return pltpu.make_async_remote_copy(
            src_ref=full.at[core, owner],
            dst_ref=full.at[core, owner],
            send_sem=p5s.at[k],
            recv_sem=p5r.at[k],
            device_id=(me, partner),
            device_id_type=MESH,
        )

    for k in range(1, msize):
        share(k).start()
    across(0).start()
    for k in range(1, msize):
        share(k).wait()
        across(k).start()
    for k in range(msize):
        across(k).wait()
    scale = 1.0 / math.sqrt(members * cells)
    for side in range(2):
        for m in range(msize):
            lo = side * nrows + m * piece
            gwi_ref[lo : lo + piece, :] = full[side, m, :, :latent].astype(F32) * scale
            acc_o[lo : lo + piece, :] = full[side, m, :, latent:].astype(F32) * scale
    turned = jnp.transpose(acc_o[...])
    gwo_ref[...] = turned[:chans]
    gb_ref[...] = turned[chans : chans + 1]
    for c in range(msize):
        for m in range(local):
            put(c, m).wait()


def on_device(hidden_codes, w_in, b_in, w_out, b_out, target, band_start):
    local, latent, cells = hidden_codes.shape
    hidden = w_in.shape[0]
    chans = w_out.shape[0]
    msize = lax.axis_size("member")
    ssize = lax.axis_size("space")
    zsize = ssize // 2
    rows = cells // LON
    lat_rows = rows * ssize
    tiles = -(-cells // 128)
    width = -(-tiles // msize) * 128
    place = jnp.arange(msize * width, dtype=jnp.int32)
    angle = ((band_start[0] + place // LON).astype(F32) + 0.5) * (
        math.pi / lat_rows
    ) - math.pi / 2
    area = jnp.where(place < cells, jnp.cos(angle), 0.0).reshape(msize, 1, width)
    nrows = hidden // 2
    piece = nrows // msize
    wide = latent + 128
    vmem = pl.BlockSpec(memory_space=pltpu.VMEM)
    dma = pltpu.SemaphoreType.DMA
    code, gwi, gwo, gb = pl.pallas_call(
        functools.partial(kernel, msize, ssize, cells),
        out_shape=(
            jax.ShapeDtypeStruct((local, cells, latent), BF16),
            jax.ShapeDtypeStruct((hidden, latent), F32),
            jax.ShapeDtypeStruct((chans, hidden), F32),
            jax.ShapeDtypeStruct((1, hidden), F32),
        ),
        in_specs=[pl.BlockSpec(memory_space=pl.ANY)] + [vmem] * 6,
        out_specs=(pl.BlockSpec(memory_space=pl.ANY),) + (vmem,) * 3,
        scratch_shapes=[
            pltpu.VMEM((msize, local, width, latent), BF16),
            pltpu.VMEM((msize, chans, width), BF16),
            pltpu.VMEM((msize, local, hidden, width), BF16),
            pltpu.VMEM((msize, local, hidden, width), F32),
            pltpu.VMEM((msize, local, chans, width), BF16),
            pltpu.VMEM((msize, local, chans, width), BF16),
            pltpu.VMEM((msize, local, chans, width), BF16),
            pltpu.VMEM((msize, local, chans, width), BF16),
            pltpu.VMEM((hidden, latent), F32),
            pltpu.VMEM((hidden, 128), F32),
            pltpu.VMEM((hidden, 128), F32),
            pltpu.VMEM((nrows, wide), BF16),
            pltpu.VMEM((nrows, wide), BF16),
            pltpu.VMEM((msize, piece, wide), BF16),
            pltpu.VMEM((msize, piece, wide), BF16),
            pltpu.VMEM((zsize, piece, wide), BF16),
            pltpu.VMEM((2, msize, piece, wide), BF16),
            dma((msize,)),
            dma((msize,)),
            dma((msize,)),
            dma((msize,)),
            dma((2,)),
            dma((msize,)),
            dma((msize,)),
            dma((zsize,)),
            dma((zsize,)),
            dma((msize,)),
            dma((msize,)),
            dma((msize,)),
            dma((msize,)),
            pltpu.VMEM((latent, hidden), BF16),
            pltpu.VMEM((hidden, chans), BF16),
            pltpu.VMEM((hidden, 128), F32),
            pltpu.VMEM((chans, 128), F32),
            dma((msize, local)),
            dma((msize, local)),
        ],
        compiler_params=pltpu.CompilerParams(
            collective_id=0, has_side_effects=True, vmem_limit_bytes=67043328
        ),
    )(
        jnp.swapaxes(hidden_codes, 1, 2),
        w_in,
        b_in[None, :],
        w_out,
        b_out[None, :],
        target,
        area,
    )
    return jnp.swapaxes(code, 1, 2), gwi, gwo, gb[0]


def solution(mesh):
    in_specs = (P("member", None, "space"), P(), P(), P(), P(), P(None, "space"), P("space"))
    out_specs = (P("member", None, "space"), P(), P(), P())
    return jax.shard_map(
        on_device, mesh=mesh, in_specs=in_specs, out_specs=out_specs, check_vma=False
    )
```
